32 devices in a mesh: seq: 8 (over z, x), head: 4 (over y, core).
Axes of the slice: x: 2, y: 2, z: 4, core: 2. Of those that a mesh axis runs over, the one named last changes fastest.
Arguments:
- x_in: bfloat16 [4096, 5120], P('seq', 'head'), may hold values from -9 to 9
- z_gate: bfloat16 [4096, 5120], P('seq', 'head'), may hold values from -6 to 6
- bc_in: bfloat16 [4096, 256], P('seq'), may hold values from -6 to 6
- conv_x: float32 [4, 5120], P(None, 'head'), may hold values from -3 to 3
- conv_bc: float32 [4, 256], replicated, may hold values from -3 to 3
- dt_raw: float32 [80, 4096], P('head', 'seq'), may hold values from -3 to 3
- dt_bias: float32 [80], P('head'), may hold values from -3.3 to 0.3
- a_log: float32 [80], P('head'), may hold values from -25 to -1
- skip_d: float32 [80], P('head'), may hold values from 0.5 to 1.5
- norm_weight: float32 [5120], replicated, may hold values from 0.5 to 1.5
- w_out: bfloat16 [5120, 2560], P('head'), may hold values from -0.078125 to 0.078125
Outputs:
- mixed_out: bfloat16 [4096, 2560], P(('seq', 'head'))
The draws below stay inside these ranges and needn't reach their ends.
All inputs are finite; a program needn't handle non-finite values.
Results may differ from the reference program's by a relative error of at most 0.014.
Values may be sent and summed in bfloat16 or wider, within the bound.
A program may use at most 128 MiB of HBM per device.

```python
import jax
import jax.numpy as jnp
from jax import lax

D_MODEL = 2560
HEADS = 80
HEAD_DIM = 64
STATE = 128
CONV = 4
GROUP = 128
D_INNER = 5120
TOKENS = 4096


def head_law(key):
    slow_share = 0.5
    slow = jax.random.uniform(jax.random.fold_in(key, 11), (HEADS,)) < slow_share
    kappa = jax.random.uniform(jax.random.fold_in(key, 12), (HEADS,), jnp.float32, 0.3, 1.5)
    fast_rate = jax.random.uniform(jax.random.fold_in(key, 13), (HEADS,), jnp.float32, 0.03, 0.06)
    return (slow, kappa, fast_rate)


def draw_a_log(key, part):
    slow, kappa, fast_rate = head_law(key)
    rate = jnp.where(slow, kappa / (0.05 * TOKENS), fast_rate)
    return jnp.log(rate).astype(jnp.float32)


def draw_dt_bias(key, part):
    slow, kappa, fast_rate = head_law(key)
    offset = jax.random.uniform(jax.random.fold_in(key, 14), (HEADS,), jnp.float32, -0.3, 0.3)
    return (jnp.where(slow, -3.0, 0.0) + offset).astype(jnp.float32)


def draw_x_in(key, part):
    channel = jnp.arange(D_INNER).astype(jnp.float32) / (D_INNER - 1)
    base = jnp.clip(jax.random.normal(jax.random.fold_in(key, 22), (TOKENS, D_INNER), jnp.float32), -6.0, 6.0)
    scale = 0.5 * 3.0 ** channel
    return (base * scale[None, :]).astype(jnp.bfloat16)


def steps_of(key, dims, split, smallest, largest):
    level, own = 1.0, jax.random.fold_in(key, 6)
    for dim, parts in split:
        steps = jnp.exp(jax.random.uniform(jax.random.fold_in(own, dim), (parts,), jnp.float32, smallest / len(split), largest / len(split)))
        level = level * jnp.repeat(steps, dims[dim] // parts).reshape([-1 if axis == dim else 1 for axis in range(len(dims))])
    return level


def gaussian(own_key, dims, deviation, most, split=(), held_as=jnp.bfloat16):
    entries = jax.random.normal(own_key, dims, jnp.float32) * deviation
    if len(split) > 0:
        entries = steps_of(own_key, dims, split, -0.22, 0.18) * entries
    return jnp.clip(entries, min=-most, max=most).astype(held_as)


def setup_inputs(seed: int = 0) -> dict:
    keys = jax.random.split(jax.random.key(seed), 12)
    return {
        "x_in": draw_x_in(jax.random.fold_in(keys[11], 71), 0),
        "z_gate": gaussian(keys[1], (TOKENS, D_INNER), 1.0, 6.0, ((0, 8), (1, 4))),
        "bc_in": gaussian(keys[2], (TOKENS, 2 * STATE), 1.0, 6.0, ((0, 8),)),
        "conv_x": gaussian(keys[3], (CONV, D_INNER), 0.5, 3.0, ((1, 4),), jnp.float32),
        "conv_bc": gaussian(keys[4], (CONV, 2 * STATE), 0.5, 3.0, (), jnp.float32),
        "dt_raw": gaussian(keys[5], (HEADS, TOKENS), 0.5, 3.0, ((0, 4), (1, 8)), jnp.float32),
        "dt_bias": draw_dt_bias(jax.random.fold_in(keys[11], 71), 0),
        "a_log": draw_a_log(jax.random.fold_in(keys[11], 71), 0),
        "skip_d": jnp.clip(0.5 + 1.0 * jax.random.uniform(keys[8], (HEADS,), jnp.float32) ** steps_of(keys[8], (HEADS,), ((0, 4),), -0.2, 0.2), 0.5, 1.5),
        "norm_weight": jnp.clip(1.0 + 0.1 * jax.random.normal(keys[9], (D_INNER,), jnp.float32), 0.5, 1.5),
        "w_out": gaussian(keys[10], (D_INNER, D_MODEL), D_INNER ** -0.5, 0.078125, ((0, 4),)),
    }


def causal_conv(source, kernel):
    length = source.shape[0]
    padded = jnp.pad(source.astype(jnp.float32), ((CONV - 1, 0), (0, 0)))
    summed = kernel[0] * padded[0:length]
    for k in range(1, CONV):
        summed = summed + kernel[k] * padded[k:k + length]
    return jax.nn.silu(summed).astype(jnp.bfloat16)

def reference(x_in, z_gate, bc_in, conv_x, conv_bc, dt_raw, dt_bias, a_log, skip_d, norm_weight, w_out):
    highest = lax.Precision.HIGHEST
    xs_all = causal_conv(x_in, conv_x)
    bcs_all = causal_conv(bc_in, conv_bc)
    step_size = jax.nn.softplus(dt_raw + dt_bias[:, None])
    log_decay = step_size * (-jnp.exp(a_log))[:, None]
    nblock = TOKENS // GROUP
    x_blocks = xs_all.reshape(nblock, GROUP, HEADS, HEAD_DIM)
    b_blocks = bcs_all[:, :STATE].reshape(nblock, GROUP, STATE)
    c_blocks = bcs_all[:, STATE:].reshape(nblock, GROUP, STATE)
    d_blocks = step_size.reshape(HEADS, nblock, GROUP).transpose(1, 0, 2)
    l_blocks = log_decay.reshape(HEADS, nblock, GROUP).transpose(1, 0, 2)
    causal = jnp.arange(GROUP)[:, None] >= jnp.arange(GROUP)[None, :]

    def group_step(running, blocks):
        x_blk, b_blk, c_blk, d_blk, l_blk = blocks
        cumulative = jnp.cumsum(l_blk, axis=1)
        segment = cumulative[:, :, None] - cumulative[:, None, :]
        decays = jnp.where(causal, jnp.exp(jnp.where(causal, segment, 0.0)), 0.0)
        c_dot_b = jnp.dot(c_blk.astype(jnp.float32), b_blk.astype(jnp.float32).T, precision=highest)
        mixer = (c_dot_b[None] * decays * d_blk[:, None, :]).astype(jnp.bfloat16)
        mixer = lax.optimization_barrier(mixer)
        y_diag = jnp.einsum('hts,shp->thp', mixer.astype(jnp.float32), x_blk.astype(jnp.float32), precision=highest)
        entering = lax.optimization_barrier(running.astype(jnp.bfloat16))
        y_off = jnp.einsum('tn,hpn->thp', c_blk.astype(jnp.float32), entering.astype(jnp.float32), precision=highest)
        y_off = y_off * jnp.exp(cumulative).T[:, :, None]
        output = y_diag + y_off + skip_d[None, :, None] * x_blk.astype(jnp.float32)
        to_end = jnp.exp(cumulative[:, -1:] - cumulative) * d_blk
        scaled = (x_blk.astype(jnp.float32) * to_end.T[:, :, None]).astype(jnp.bfloat16)
        scaled = lax.optimization_barrier(scaled)
        local_term = jnp.einsum('shp,sn->hpn', scaled.astype(jnp.float32), b_blk.astype(jnp.float32), precision=highest)
        running = jnp.exp(cumulative[:, -1])[:, None, None] * running + local_term
        return (running, output)
    start_state = jnp.zeros((HEADS, HEAD_DIM, STATE), jnp.float32)
    final_state, outputs = lax.scan(group_step, start_state, (x_blocks, b_blocks, c_blocks, d_blocks, l_blocks))
    y_all = outputs.reshape(TOKENS, D_INNER)
    gated = (y_all * jax.nn.silu(z_gate.astype(jnp.float32))).astype(jnp.bfloat16)
    gated_f = gated.astype(jnp.float32)
    sum_squares = lax.optimization_barrier(jnp.sum(gated_f * gated_f, axis=1))
    inv_rms = lax.rsqrt(sum_squares / D_INNER + 1e-05)
    normed = (gated_f * inv_rms[:, None] * norm_weight[None, :]).astype(jnp.bfloat16)
    return jnp.dot(normed, w_out, preferred_element_type=jnp.float32).astype(jnp.bfloat16)
```

```python
import functools

import jax
import jax.numpy as jnp
from jax import lax
from jax.experimental import pallas as pl
from jax.experimental.pallas import tpu as pltpu
from jax.sharding import PartitionSpec as P

HEAD_DIM = 64
STATE = 128
CONV = 4
GROUP = 128
LANES = 128
HALO = 16
COLS = 512
EPSILON = 1e-05
MESH = pl.DeviceIdType.MESH
F32 = jnp.float32
BF16 = jnp.bfloat16
HIGH = lax.Precision.HIGHEST


def silu(v):
    half = 0.5 * v
    return half + half * jnp.tanh(half)


def dot(a, b):
    return jnp.dot(a, b, preferred_element_type=F32)


def dot_nt(a, b):
    return lax.dot_general(a, b, (((1,), (1,)), ((), ())), precision=HIGH, preferred_element_type=F32)


def split(v):
    high = v.astype(BF16)
    return high, (v - high.astype(F32)).astype(BF16)


def kernel(
    n_seq, n_head, d_inner,
    x_hbm, z_hbm, bc_hbm, w_hbm, convx, convbc, dt_raw, dt_bias, a_log, skip, gain,
    out,
    xv, zv, bcv, wv, hx, hbc, xf, bcf, xs, cs, bt, dts, las, cum_t, row_t, te_hi, te_lo, ef_hi, ef_lo, emat, skipx,
    exp_f, pre, est, hl, dm, hpart, dpart, prev, psend, csend, inc, aa, bf, gn, acc,
    tosib, fromsib, keep, ysend, yrecv, ssend, srecv,
    load_sem, halo_send, halo_recv, a_send, a_recv, d_send, d_recv, b_send, b_recv, c_send, c_recv,
    sib_send, sib_recv, y_send, y_recv, s_send, s_recv,
):
    rows, width = xv.shape
    heads = dt_raw.shape[0]
    hp = las.shape[0]
    nb, nj = rows // GROUP, width // LANES
    d_model = wv.shape[1]
    own = out.shape[0]
    ncol = d_model // COLS
    n_chip = n_head // 2
    s = lax.axis_index("seq")
    hid = lax.axis_index("head")
    par, pair, npair = lax.rem(s, 2), s // 2, n_seq // 2
    partner = s + 1 - 2 * par
    chip, core = hid // 2, lax.rem(hid, 2)
    sibling = hid + 1 - 2 * core

    loads = [
        pltpu.make_async_copy(bc_hbm, bcv, load_sem.at[0]),
        pltpu.make_async_copy(x_hbm, xv, load_sem.at[1]),
        pltpu.make_async_copy(z_hbm, zv, load_sem.at[2]),
        pltpu.make_async_copy(w_hbm, wv, load_sem.at[3]),
    ]
    for load in loads:
        load.start()

    barrier = pltpu.get_barrier_semaphore()
    count = 0
    for off in (-2, -1, 1, 2):
        there = jnp.logical_and(s + off >= 0, s + off < n_seq)

        @pl.when(there)
        def _():
            pl.semaphore_signal(barrier, inc=1, device_id={"seq": s + off}, device_id_type=MESH)

        count = count + jnp.where(there, 1, 0)
    for d in range(1, n_head):
        pl.semaphore_signal(
            barrier, inc=1, device_id={"head": lax.rem(hid + d, n_head)}, device_id_type=MESH
        )
    pl.semaphore_wait(barrier, count + n_head - 1)

    def remote(src, dst, send, recv, axis, to):
        return pltpu.make_async_remote_copy(
            src_ref=src, dst_ref=dst, send_sem=send, recv_sem=recv,
            device_id={axis: to}, device_id_type=MESH,
        )

    halo_x = remote(x_hbm.at[pl.ds(rows - HALO, HALO)], hx, halo_send.at[0], halo_recv.at[0], "seq", s + 1)
    halo_b = remote(bc_hbm.at[pl.ds(rows - HALO, HALO)], hbc, halo_send.at[1], halo_recv.at[1], "seq", s + 1)

    @pl.when(s < n_seq - 1)
    def _():
        halo_b.start()
        halo_x.start()

    @pl.when(s == 0)
    def _():
        hx[...] = jnp.zeros_like(hx)
        hbc[...] = jnp.zeros_like(hbc)

    @pl.when(pair == 0)
    def _():
        prev[...] = jnp.zeros_like(prev)

    raw = dt_raw[...] + dt_bias[...]
    dt = jnp.maximum(raw, 0.0) + jnp.log(1.0 + jnp.exp(-jnp.abs(raw)))
    dts[...] = jnp.ones_like(dts)
    las[...] = jnp.zeros_like(las)
    dts[0:heads, :] = dt
    las[0:heads, :] = dt * (-jnp.exp(a_log[...]))
    ti = lax.broadcasted_iota(jnp.int32, (GROUP, GROUP), 0)
    si = lax.broadcasted_iota(jnp.int32, (GROUP, GROUP), 1)
    causal = ti >= si
    tri = causal.astype(F32)
    eye = (ti == si).astype(F32)
    emat[...] = (
        lax.broadcasted_iota(jnp.int32, (hp, width), 1) // HEAD_DIM
        == lax.broadcasted_iota(jnp.int32, (hp, width), 0)
    ).astype(F32).astype(BF16)
    for c in range(nb):
        blk = slice(c * GROUP, (c + 1) * GROUP)
        dt_c, la_c = dts[:, blk], las[:, blk]
        cum = dot_nt(tri, la_c)
        cum_t[blk, :] = cum
        row_t[c] = dot_nt(la_c, tri) - jnp.log(dt_c)
        te = jnp.exp(cum[GROUP - 1 :, :] - cum) * dot_nt(eye, dt_c)
        te_hi[blk, :], te_lo[blk, :] = split(te)
        ef_hi[blk, :], ef_lo[blk, :] = split(jnp.exp(cum))
    sk = jnp.where(
        lax.broadcasted_iota(jnp.int32, (heads, width), 1) // HEAD_DIM
        == lax.broadcasted_iota(jnp.int32, (heads, width), 0),
        skip[...], 0.0,
    )
    skipx[...] = jnp.broadcast_to(jnp.sum(sk, axis=0, keepdims=True), skipx.shape)

    loads[0].wait()
    loads[1].wait()

    @pl.when(s > 0)
    def _():
        halo_b.wait_recv()
        halo_x.wait_recv()

    bcf[0:8, :] = hbc[...].astype(F32)[HALO - 8 :]
    bcf[8:, :] = bcv[...].astype(F32)
    conv = convbc[0:1, :] * bcf[pl.ds(9 - CONV, rows), :]
    for k in range(1, CONV):
        conv = conv + convbc[k : k + 1, :] * bcf[pl.ds(9 - CONV + k, rows), :]
    bcs = silu(conv).astype(BF16)
    cs[...] = bcs[:, STATE:]
    for c in range(nb):
        bt[c] = bcs[c * GROUP : (c + 1) * GROUP, :STATE].astype(F32).T.astype(BF16)

    def sends_a(j):
        return (
            remote(hl.at[j], hpart.at[j], a_send.at[j], a_recv.at[j], "seq", partner),
            remote(dm.at[j], dpart.at[j], d_send.at[j], d_recv.at[j], "seq", partner),
        )

    def send_b(j):
        return remote(psend.at[j], prev.at[j], b_send.at[j], b_recv.at[j], "seq", s + 2)

    def send_c(j):
        return remote(csend.at[j], inc.at[j], c_send.at[j], c_recv.at[j], "seq", partner)

    def lanes_of(j):
        return pl.ds(pl.multiple_of(j * LANES, LANES), LANES)

    def own_state(j, carry):
        ln = lanes_of(j)
        xf[0:8, :] = hx[:, ln].astype(F32)[HALO - 8 :]
        xf[8:, :] = xv[:, ln].astype(F32)
        cx = convx[:, ln]
        total = cx[0:1, :] * xf[pl.ds(9 - CONV, rows), :]
        for k in range(1, CONV):
            total = total + cx[k : k + 1, :] * xf[pl.ds(9 - CONV + k, rows), :]
        xb = silu(total).astype(BF16)
        xs[:, ln] = xb
        em = emat[:, ln]
        u = (xb.astype(F32) * (dot(te_hi[...], em) + dot(te_lo[...], em))).astype(BF16)
        ef = dot(ef_hi[...], em) + dot(ef_lo[...], em)
        exp_f[:, ln] = ef
        run = jnp.zeros((STATE, LANES), F32)
        carried = jnp.ones((1, LANES), F32)
        for c in range(nb):
            blk = slice(c * GROUP, (c + 1) * GROUP)
            est[c, :, ln] = run.astype(BF16)
            pre[c, :, ln] = jnp.broadcast_to(carried, (8, LANES))
            decay = ef[(c + 1) * GROUP - 1 : (c + 1) * GROUP, :]
            run = decay * run + dot(bt[c], u[blk])
            carried = carried * decay
        hl[j] = run.astype(BF16)
        dm[j] = jnp.broadcast_to(carried, (8, LANES))

        @pl.when(lax.rem(j, 2) != par)
        def _():
            for copy in sends_a(j):
                copy.start()

        return carry

    lax.fori_loop(0, nj, own_state, 0)
    loads[2].wait()

    lane = lax.broadcasted_iota(jnp.int32, (GROUP, LANES), 1)

    def block(c, carry):
        tk = pl.ds(pl.multiple_of(c * GROUP, GROUP), GROUP)
        c_c = cs[tk, :]
        cb = dot(c_c, bt[c])
        cum = cum_t[tk, :]
        row = row_t[c]
        for j in range(nj):
            ln = slice(j * LANES, (j + 1) * LANES)
            x = xs[tk, ln]
            y = skipx[0:1, ln] * x.astype(F32)
            for k in range(2):
                h = 2 * j + k
                seg = cum[:, h : h + 1] - row[h : h + 1, :]
                g = (cb * jnp.exp(jnp.where(causal, seg, -1e30))).astype(BF16)
                y = y + dot(g, jnp.where((lane < HEAD_DIM) == (k == 0), x, jnp.zeros_like(x)))
            ef = exp_f[tk, ln]
            y = y + ef * dot(c_c, est[c, :, ln])
            sz = silu(zv[tk, ln].astype(F32))
            aa[tk, ln] = y * sz
            bf[tk, ln] = ef * pre[c, 0:1, ln] * sz
        return carry

    early = jnp.minimum(pair, nb)
    lax.fori_loop(0, early, block, 0)

    def serve(i, carry):
        j = 2 * i + par
        for copy in sends_a(j):
            copy.wait_recv()

        @pl.when(pair > 0)
        def _():
            send_b(j).wait_recv()

        first = par == 0
        h_me, h_other = hl[j].astype(F32), hpart[j].astype(F32)
        d_me, d_other = dm[j, 0:1, :], dpart[j, 0:1, :]
        h0, h1 = jnp.where(first, h_me, h_other), jnp.where(first, h_other, h_me)
        d0, d1 = jnp.where(first, d_me, d_other), jnp.where(first, d_other, d_me)
        in0 = prev[j].astype(F32)
        in1 = d0 * in0 + h0

        @pl.when(pair < npair - 1)
        def _():
            psend[j] = (d1 * in1 + h1).astype(BF16)
            send_b(j).start()

        csend[j] = jnp.where(first, in1, in0).astype(BF16)
        send_c(j).start()
        inc[j] = jnp.where(first, in0, in1).astype(BF16)
        return carry

    lax.fori_loop(0, nj // 2, serve, 0)
    lax.fori_loop(early, nb, block, 0)

    acc[...] = jnp.zeros_like(acc)

    def gate(j):
        ln = lanes_of(j)
        g = (aa[:, ln] + bf[:, ln] * dot(cs[...], inc[j])).astype(BF16).astype(F32)
        acc[...] += g * g
        gn[:, ln] = (g * gain[hid, :, ln]).astype(BF16)

    def gate_own(i, carry):
        gate(2 * i + par)
        return carry

    def gate_sent(i, carry):
        j = 2 * i + 1 - par
        send_c(j).wait_recv()
        gate(j)
        return carry

    lax.fori_loop(0, nj // 2, gate_own, 0)
    lax.fori_loop(0, nj // 2, gate_sent, 0)
    loads[3].wait()

    far = (n_chip - 1) * ncol

    def sib(e):
        return remote(tosib.at[e], fromsib.at[e], sib_send.at[e], sib_recv.at[e], "head", sibling)

    def chip_of(e):
        return lax.rem(chip + e // ncol + 1, n_chip)

    def over(e):
        return remote(ysend.at[e], yrecv.at[e], y_send.at[e], y_recv.at[e], "head", chip_of(e) * 2 + core)

    def project(e):
        base = chip_of(e) * 2
        n = lax.rem(e, ncol)
        theirs = gn[pl.ds(pl.multiple_of((base + 1 - core) * own, own), own), :]
        mine = gn[pl.ds(pl.multiple_of((base + core) * own, own), own), :]
        part = dot(
            jnp.concatenate([theirs, mine], axis=0),
            wv[:, pl.ds(pl.multiple_of(n * COLS, COLS), COLS)],
        )
        tosib[e] = part[:own].astype(BF16)
        sib(e).start()
        keep[e] = part[own:]

    def forward(e):
        sib(e).wait_recv()
        ysend[e] = (keep[e] + fromsib[e].astype(F32)).astype(BF16)
        over(e).start()

    def ssq_send(d):
        to = lax.rem(hid + d, n_head)
        return remote(ssend.at[to], srecv.at[d], s_send.at[d], s_recv.at[d], "head", to)

    def step(e, carry):
        project(e)

        @pl.when(jnp.logical_and(e > 0, e <= far))
        def _():
            forward(e - 1)

        return carry

    lax.fori_loop(0, far + ncol, step, 0)

    for b in range(n_head):
        flipped = acc[b * own : (b + 1) * own, :].T
        ssend[b] = jnp.broadcast_to(jnp.sum(flipped, axis=0, keepdims=True), ssend.shape[1:])
    for d in range(1, n_head):
        ssq_send(d).start()
    ssq = ssend[hid]
    for d in range(1, n_head):
        ssq_send(d).wait_recv()
        ssq = ssq + srecv[d]
    inv = lax.rsqrt(ssq[0:1, :] / d_inner + EPSILON)
    inv = jnp.broadcast_to(inv, (LANES, own)).T[:, 0:1]

    def finish(n, carry):
        e = far + n
        sib(e).wait_recv()
        total = keep[e] + fromsib[e].astype(F32)
        for r in range(n_chip - 1):
            over(r * ncol + n).wait_recv()
            total = total + yrecv[r * ncol + n].astype(F32)
        out[:, pl.ds(pl.multiple_of(n * COLS, COLS), COLS)] = (total * inv).astype(BF16)
        return carry

    lax.fori_loop(0, ncol, finish, 0)

    @pl.when(s < n_seq - 1)
    def _():
        halo_b.wait_send()
        halo_x.wait_send()

    def left(i, carry):
        for copy in sends_a(2 * i + 1 - par):
            copy.wait_send()
        send_c(2 * i + par).wait_send()

        @pl.when(pair < npair - 1)
        def _():
            send_b(2 * i + par).wait_send()

        return carry

    lax.fori_loop(0, nj // 2, left, 0)
    for e in range(far + ncol):
        sib(e).wait_send()
    for e in range(far):
        over(e).wait_send()
    for d in range(1, n_head):
        ssq_send(d).wait_send()


def solution(mesh):
    n_seq, n_head = mesh.shape["seq"], mesh.shape["head"]

    def per_device(x_in, z_gate, bc_in, conv_x, conv_bc, dt_raw, dt_bias, a_log, skip_d, norm_weight, w_out):
        rows, width = x_in.shape
        heads = dt_raw.shape[0]
        d_model = w_out.shape[1]
        hp = -(-heads // 32) * 32
        nb, nj, own, ncol = rows // GROUP, width // LANES, rows // n_head, d_model // COLS
        every, far = (n_head // 2) * ncol, (n_head // 2 - 1) * ncol
        assert nj % 2 == 0 and n_seq % 2 == 0 and n_head % 2 == 0 and own == LANES
        hbm, vmem = pl.BlockSpec(memory_space=pl.ANY), pl.BlockSpec(memory_space=pltpu.VMEM)
        dma = pltpu.SemaphoreType.DMA
        scratch = [
            ((rows, width), BF16), ((rows, width), BF16), ((rows, 2 * STATE), BF16), (w_out.shape, BF16),
            ((HALO, width), BF16), ((HALO, 2 * STATE), BF16),
            ((rows + 8, LANES), F32), ((rows + 8, 2 * STATE), F32),
            ((rows, width), BF16), ((rows, STATE), BF16), ((nb, STATE, GROUP), BF16),
            ((hp, rows), F32), ((hp, rows), F32), ((rows, hp), F32), ((nb, hp, GROUP), F32),
            ((rows, hp), BF16), ((rows, hp), BF16), ((rows, hp), BF16), ((rows, hp), BF16),
            ((hp, width), BF16), ((8, width), F32),
            ((rows, width), F32), ((nb, 8, width), F32), ((nb, STATE, width), BF16),
            ((nj, STATE, LANES), BF16), ((nj, 8, LANES), F32), ((nj, STATE, LANES), BF16), ((nj, 8, LANES), F32),
            ((nj, STATE, LANES), BF16), ((nj, STATE, LANES), BF16), ((nj, STATE, LANES), BF16),
            ((nj, STATE, LANES), BF16),
            ((rows, width), F32), ((rows, width), F32), ((rows, width), BF16), ((rows, LANES), F32),
            ((every, own, COLS), BF16), ((every, own, COLS), BF16), ((every, own, COLS), F32),
            ((far, own, COLS), BF16), ((far, own, COLS), BF16),
            ((n_head, 8, own), F32), ((n_head, 8, own), F32),
        ]
        sems = [4, 2, 2] + [nj] * 8 + [every, every, far, far, n_head, n_head]
        return pl.pallas_call(
            functools.partial(kernel, n_seq, n_head, norm_weight.shape[0]),
            out_shape=jax.ShapeDtypeStruct((own, d_model), BF16),
            in_specs=[hbm] * 4 + [vmem] * 7,
            out_specs=vmem,
            scratch_shapes=[pltpu.VMEM(*one) for one in scratch] + [dma((k,)) for k in sems],
            compiler_params=pltpu.CompilerParams(
                collective_id=0, has_side_effects=True, vmem_limit_bytes=60 * 2**20
            ),
        )(
            x_in, z_gate, bc_in, w_out, conv_x, conv_bc, dt_raw, dt_bias[:, None], a_log[:, None],
            skip_d[:, None], norm_weight.reshape(n_head, 1, width),
        )

    in_specs = (
        P("seq", "head"), P("seq", "head"), P("seq", None), P(None, "head"), P(), P("head", "seq"),
        P("head"), P("head"), P("head"), P(), P("head", None),
    )
    return jax.shard_map(
        per_device, mesh=mesh, in_specs=in_specs, out_specs=P(("seq", "head"), None), check_vma=False
    )
```

```python
import functools

import jax
import jax.numpy as jnp
from jax import lax
from jax.experimental import pallas as pl
from jax.experimental.pallas import tpu as pltpu
from jax.sharding import PartitionSpec as P

HEAD_DIM = 64
STATE = 128
CONV = 4
GROUP = 128
LANES = 128
HALO = 16
COLS = 256
LAG = 4
EPSILON = 1e-05
MESH = pl.DeviceIdType.MESH
F32 = jnp.float32
BF16 = jnp.bfloat16
HIGH = lax.Precision.HIGHEST


def silu(v):
    half = 0.5 * v
    return half + half * jnp.tanh(half)


def dot(a, b):
    return jnp.dot(a, b, preferred_element_type=F32)


def dot_nt(a, b):
    return lax.dot_general(a, b, (((1,), (1,)), ((), ())), precision=HIGH, preferred_element_type=F32)


def split(v):
    high = v.astype(BF16)
    return high, (v - high.astype(F32)).astype(BF16)


def kernel(
    n_seq, n_head, d_inner,
    x_hbm, z_hbm, bc_hbm, w_hbm, convx, convbc, dt_raw, dt_bias, a_log, skip, gain,
    out,
    xv, zv, bcv, wv, hx, hbc, xf, bcf, xs, cs, bt, dts, las, cum_t, row_t, te_b, end_hi, end_lo, ef_hi, ef_lo, emat, skipx,
    pre, est, hl, dm, hpart, dpart, prev, psend, csend, inc, aa, bf, gn, acc,
    tosib, fromsib, keep, ysend, yrecv, ssend, srecv,
    load_sem, halo_send, halo_recv, a_send, a_recv, d_send, d_recv, b_send, b_recv, c_send, c_recv,
    sib_send, sib_recv, y_send, y_recv, s_send, s_recv,
):
    rows, width = xv.shape
    heads = dt_raw.shape[0]
    hp = las.shape[0]
    nb, nj = rows // GROUP, width // LANES
    d_model = wv.shape[1]
    own = out.shape[0]
    ncol = d_model // COLS
    n_chip = n_head // 2
    s = lax.axis_index("seq")
    hid = lax.axis_index("head")
    par, pair, npair = lax.rem(s, 2), s // 2, n_seq // 2
    partner = s + 1 - 2 * par
    chip, core = hid // 2, lax.rem(hid, 2)
    sibling = hid + 1 - 2 * core

    loads = [
        pltpu.make_async_copy(bc_hbm, bcv, load_sem.at[0]),
        pltpu.make_async_copy(x_hbm, xv, load_sem.at[1]),
        pltpu.make_async_copy(z_hbm, zv, load_sem.at[2]),
        pltpu.make_async_copy(w_hbm, wv, load_sem.at[3]),
    ]
    for load in loads:
        load.start()

    barrier = pltpu.get_barrier_semaphore()
    count = 0
    for off in (-2, -1, 1, 2):
        there = jnp.logical_and(s + off >= 0, s + off < n_seq)

        @pl.when(there)
        def _():
            pl.semaphore_signal(barrier, inc=1, device_id={"seq": s + off}, device_id_type=MESH)

        count = count + jnp.where(there, 1, 0)
    for d in range(1, n_head):
        pl.semaphore_signal(
            barrier, inc=1, device_id={"head": lax.rem(hid + d, n_head)}, device_id_type=MESH
        )
    pl.semaphore_wait(barrier, count + n_head - 1)

    def remote(src, dst, send, recv, axis, to):
        return pltpu.make_async_remote_copy(
            src_ref=src, dst_ref=dst, send_sem=send, recv_sem=recv,
            device_id={axis: to}, device_id_type=MESH,
        )

    halo_x = remote(x_hbm.at[pl.ds(rows - HALO, HALO)], hx, halo_send.at[0], halo_recv.at[0], "seq", s + 1)
    halo_b = remote(bc_hbm.at[pl.ds(rows - HALO, HALO)], hbc, halo_send.at[1], halo_recv.at[1], "seq", s + 1)

    @pl.when(s < n_seq - 1)
    def _():
        halo_b.start()
        halo_x.start()

    @pl.when(s == 0)
    def _():
        hx[...] = jnp.zeros_like(hx)
        hbc[...] = jnp.zeros_like(hbc)

    @pl.when(pair == 0)
    def _():
        prev[...] = jnp.zeros_like(prev)

    same = lax.broadcasted_iota(jnp.int32, (heads, heads), 0) == lax.broadcasted_iota(jnp.int32, (heads, heads), 1)

    def column(row):
        return jnp.sum(jnp.where(same, row[...], 0.0), axis=1, keepdims=True)

    raw = dt_raw[...] + column(dt_bias)
    dt = jnp.maximum(raw, 0.0) + jnp.log(1.0 + jnp.exp(-jnp.abs(raw)))
    dts[...] = jnp.ones_like(dts)
    las[...] = jnp.zeros_like(las)
    dts[0:heads, :] = dt
    las[0:heads, :] = dt * (-jnp.exp(column(a_log)))
    ti = lax.broadcasted_iota(jnp.int32, (GROUP, GROUP), 0)
    si = lax.broadcasted_iota(jnp.int32, (GROUP, GROUP), 1)
    causal = ti >= si
    tri = causal.astype(F32)
    eye = (ti == si).astype(F32)
    emat[...] = (
        lax.broadcasted_iota(jnp.int32, (hp, width), 1) // HEAD_DIM
        == lax.broadcasted_iota(jnp.int32, (hp, width), 0)
    ).astype(F32).astype(BF16)
    for c in range(nb):
        blk = slice(c * GROUP, (c + 1) * GROUP)
        dt_c, la_c = dts[:, blk], las[:, blk]
        cum = dot_nt(tri, la_c)
        cum_t[blk, :] = cum
        row_t[c] = dot_nt(la_c, tri) - jnp.log(dt_c)
        te = jnp.exp(cum[GROUP - 1 :, :] - cum) * dot_nt(eye, dt_c)
        te_b[blk, :] = te.astype(BF16)
        grown = jnp.exp(cum)
        ef_hi[blk, :], ef_lo[blk, :] = split(grown)
        end_hi[c], end_lo[c] = split(jnp.broadcast_to(grown[GROUP - 1 :, :], end_hi.shape[1:]))
    sk = jnp.where(
        lax.broadcasted_iota(jnp.int32, (heads, width), 1) // HEAD_DIM
        == lax.broadcasted_iota(jnp.int32, (heads, width), 0),
        column(skip), 0.0,
    )
    skipx[...] = jnp.broadcast_to(jnp.sum(sk, axis=0, keepdims=True), skipx.shape)

    loads[0].wait()
    loads[1].wait()

    @pl.when(s > 0)
    def _():
        halo_b.wait_recv()
        halo_x.wait_recv()

    bcf[0:8, :] = hbc[...].astype(F32)[HALO - 8 :]
    bcf[8:, :] = bcv[...].astype(F32)
    conv = convbc[0:1, :] * bcf[pl.ds(9 - CONV, rows), :]
    for k in range(1, CONV):
        conv = conv + convbc[k : k + 1, :] * bcf[pl.ds(9 - CONV + k, rows), :]
    bcs = silu(conv).astype(BF16)
    cs[...] = bcs[:, STATE:]
    for c in range(nb):
        bt[c] = bcs[c * GROUP : (c + 1) * GROUP, :STATE].astype(F32).T.astype(BF16)

    def sends_a(j):
        return (
            remote(hl.at[j], hpart.at[j], a_send.at[j], a_recv.at[j], "seq", partner),
            remote(dm.at[j], dpart.at[j], d_send.at[j], d_recv.at[j], "seq", partner),
        )

    def send_b(j):
        return remote(psend.at[j], prev.at[j], b_send.at[j], b_recv.at[j], "seq", s + 2)

    def send_c(j):
        return remote(csend.at[j], inc.at[j], c_send.at[j], c_recv.at[j], "seq", partner)

    def lanes_of(j):
        return pl.ds(pl.multiple_of(j * LANES, LANES), LANES)

    def serve(i, carry):
        j = 2 * i + par
        for copy in sends_a(j):
            copy.wait_recv()

        @pl.when(pair > 0)
        def _():
            send_b(j).wait_recv()

        first = par == 0
        h_me, h_other = hl[j].astype(F32), hpart[j].astype(F32)
        d_me, d_other = dm[j, 0:1, :], dpart[j, 0:1, :]
        h0, h1 = jnp.where(first, h_me, h_other), jnp.where(first, h_other, h_me)
        d0, d1 = jnp.where(first, d_me, d_other), jnp.where(first, d_other, d_me)
        in0 = prev[j].astype(F32)
        in1 = d0 * in0 + h0

        @pl.when(pair < npair - 1)
        def _():
            psend[j] = (d1 * in1 + h1).astype(BF16)
            send_b(j).start()

        csend[j] = jnp.where(first, in1, in0).astype(BF16)
        send_c(j).start()
        inc[j] = jnp.where(first, in0, in1).astype(BF16)
        return carry

    def own_state(j, carry):
        ln = lanes_of(j)
        xf[0:8, :] = hx[:, ln].astype(F32)[HALO - 8 :]
        xf[8:, :] = xv[:, ln].astype(F32)
        cx = convx[:, ln]
        total = cx[0:1, :] * xf[pl.ds(9 - CONV, rows), :]
        for k in range(1, CONV):
            total = total + cx[k : k + 1, :] * xf[pl.ds(9 - CONV + k, rows), :]
        xb = silu(total).astype(BF16)
        xs[:, ln] = xb
        em = emat[:, ln]
        u = (xb.astype(F32) * dot(te_b[...], em)).astype(BF16)
        run = jnp.zeros((STATE, LANES), F32)
        carried = jnp.ones((1, LANES), F32)
        for c in range(nb):
            blk = slice(c * GROUP, (c + 1) * GROUP)
            est[c, :, ln] = run.astype(BF16)
            pre[c, :, ln] = jnp.broadcast_to(carried, (8, LANES))
            decay = (dot(end_hi[c], em) + dot(end_lo[c], em))[0:1, :]
            run = decay * run + dot(bt[c], u[blk])
            carried = carried * decay
        hl[j] = run.astype(BF16)
        dm[j] = jnp.broadcast_to(carried, (8, LANES))

        @pl.when(lax.rem(j, 2) != par)
        def _():
            for copy in sends_a(j):
                copy.start()

        late = j - LAG

        @pl.when(jnp.logical_and(pair == 0, jnp.logical_and(late >= 0, lax.rem(late + par + 2, 2) == 0)))
        def _():
            serve(late // 2, 0)

        return carry

    lax.fori_loop(0, nj, own_state, 0)
    done = jnp.where(pair == 0, (nj - LAG + 1 - par) // 2, 0)
    loads[2].wait()

    lane = lax.broadcasted_iota(jnp.int32, (GROUP, LANES), 1)

    def block(c, carry):
        tk = pl.ds(pl.multiple_of(c * GROUP, GROUP), GROUP)
        c_c = cs[tk, :]
        cb = dot(c_c, bt[c])
        cum = cum_t[tk, :]
        row = row_t[c]
        for j in range(nj):
            ln = slice(j * LANES, (j + 1) * LANES)
            x = xs[tk, ln]
            y = skipx[0:1, ln] * x.astype(F32)
            for k in range(2):
                h = 2 * j + k
                seg = cum[:, h : h + 1] - row[h : h + 1, :]
                g = (cb * jnp.exp(jnp.where(causal, seg, -1e30))).astype(BF16)
                y = y + dot(g, jnp.where((lane < HEAD_DIM) == (k == 0), x, jnp.zeros_like(x)))
            em = emat[:, ln]
            ef = dot(ef_hi[tk, :], em) + dot(ef_lo[tk, :], em)
            y = y + ef * dot(c_c, est[c, :, ln])
            sz = silu(zv[tk, ln].astype(F32))
            aa[tk, ln] = y * sz
            bf[tk, ln] = ef * pre[c, 0:1, ln] * sz
        return carry

    early = jnp.minimum(jnp.where(pair == npair - 1, pair, jnp.maximum(pair - 1, 0)), nb - 1)
    lax.fori_loop(0, early, block, 0)

    lax.fori_loop(done, nj // 2, serve, 0)
    lax.fori_loop(early, nb, block, 0)

    acc[...] = jnp.zeros_like(acc)

    chip_rows = 2 * own

    def gate(j, r):
        ln = lanes_of(j)
        tk = pl.ds(pl.multiple_of(lax.rem(chip + r, n_chip) * chip_rows, chip_rows), chip_rows)
        g = (aa[tk, ln] + bf[tk, ln] * dot(cs[tk, :], inc[j])).astype(BF16).astype(F32)
        acc[tk, :] += g * g
        gn[tk, ln] = (g * gain[hid, :, ln]).astype(BF16)

    def gate_own(i, carry):
        for r in range(n_chip):
            gate(2 * i + par, r)
        return carry

    def gate_sent(i, carry):
        j = 2 * i + 1 - par
        send_c(j).wait_recv()
        for r in range(1, n_chip):
            gate(j, r)
        return carry

    def gate_near(i, carry):
        gate(2 * i + 1 - par, 0)
        return carry

    lax.fori_loop(0, nj // 2, gate_own, 0)
    lax.fori_loop(0, nj // 2, gate_sent, 0)
    loads[3].wait()

    far = (n_chip - 1) * ncol

    def sib(e):
        return remote(tosib.at[e], fromsib.at[e], sib_send.at[e], sib_recv.at[e], "head", sibling)

    def chip_of(e):
        return lax.rem(chip + e // ncol + 1, n_chip)

    def over(e):
        return remote(ysend.at[e], yrecv.at[e], y_send.at[e], y_recv.at[e], "head", chip_of(e) * 2 + core)

    def project(e):
        base = chip_of(e) * 2
        n = lax.rem(e, ncol)
        theirs = gn[pl.ds(pl.multiple_of((base + 1 - core) * own, own), own), :]
        mine = gn[pl.ds(pl.multiple_of((base + core) * own, own), own), :]
        part = dot(
            jnp.concatenate([theirs, mine], axis=0),
            wv[:, pl.ds(pl.multiple_of(n * COLS, COLS), COLS)],
        )
        tosib[e] = part[:own].astype(BF16)
        sib(e).start()
        keep[e] = part[own:]

    def forward(e):
        sib(e).wait_recv()
        ysend[e] = (keep[e] + fromsib[e].astype(F32)).astype(BF16)
        over(e).start()

    def ssq_send(d):
        to = lax.rem(hid + d, n_head)
        return remote(ssend.at[to], srecv.at[d], s_send.at[d], s_recv.at[d], "head", to)

    def step(e, carry):
        project(e)

        @pl.when(e > 0)
        def _():
            forward(e - 1)

        return carry

    def near(e, carry):
        project(e)
        return carry

    lax.fori_loop(0, far, step, 0)
    forward(far - 1)
    lax.fori_loop(0, nj // 2, gate_near, 0)
    lax.fori_loop(far, far + ncol, near, 0)

    for b in range(n_head):
        flipped = acc[b * own : (b + 1) * own, :].T
        ssend[b] = jnp.broadcast_to(jnp.sum(flipped, axis=0, keepdims=True), ssend.shape[1:])
    for d in range(1, n_head):
        ssq_send(d).start()
    ssq = ssend[hid]
    for d in range(1, n_head):
        ssq_send(d).wait_recv()
        ssq = ssq + srecv[d]
    inv = lax.rsqrt(ssq[0:1, :] / d_inner + EPSILON)
    inv = jnp.broadcast_to(inv, (LANES, own)).T[:, 0:1]

    def finish(n, carry):
        e = far + n
        sib(e).wait_recv()
        total = keep[e] + fromsib[e].astype(F32)
        for r in range(n_chip - 1):
            over(r * ncol + n).wait_recv()
            total = total + yrecv[r * ncol + n].astype(F32)
        out[:, pl.ds(pl.multiple_of(n * COLS, COLS), COLS)] = (total * inv).astype(BF16)
        return carry

    lax.fori_loop(0, ncol, finish, 0)

    @pl.when(s < n_seq - 1)
    def _():
        halo_b.wait_send()
        halo_x.wait_send()

    def left(i, carry):
        for copy in sends_a(2 * i + 1 - par):
            copy.wait_send()
        send_c(2 * i + par).wait_send()

        @pl.when(pair < npair - 1)
        def _():
            send_b(2 * i + par).wait_send()

        return carry

    lax.fori_loop(0, nj // 2, left, 0)
    for e in range(far + ncol):
        sib(e).wait_send()
    for e in range(far):
        over(e).wait_send()
    for d in range(1, n_head):
        ssq_send(d).wait_send()


def solution(mesh):
    n_seq, n_head = mesh.shape["seq"], mesh.shape["head"]

    def per_device(x_in, z_gate, bc_in, conv_x, conv_bc, dt_raw, dt_bias, a_log, skip_d, norm_weight, w_out):
        rows, width = x_in.shape
        heads = dt_raw.shape[0]
        d_model = w_out.shape[1]
        hp = -(-heads // 32) * 32
        nb, nj, own, ncol = rows // GROUP, width // LANES, rows // n_head, d_model // COLS
        every, far = (n_head // 2) * ncol, (n_head // 2 - 1) * ncol
        assert nj % 2 == 0 and n_seq % 2 == 0 and n_head % 2 == 0 and own == LANES
        hbm, vmem = pl.BlockSpec(memory_space=pl.ANY), pl.BlockSpec(memory_space=pltpu.VMEM)
        dma = pltpu.SemaphoreType.DMA
        scratch = [
            ((rows, width), BF16), ((rows, width), BF16), ((rows, 2 * STATE), BF16), (w_out.shape, BF16),
            ((HALO, width), BF16), ((HALO, 2 * STATE), BF16),
            ((rows + 8, LANES), F32), ((rows + 8, 2 * STATE), F32),
            ((rows, width), BF16), ((rows, STATE), BF16), ((nb, STATE, GROUP), BF16),
            ((hp, rows), F32), ((hp, rows), F32), ((rows, hp), F32), ((nb, hp, GROUP), F32),
            ((rows, hp), BF16), ((nb, 16, hp), BF16), ((nb, 16, hp), BF16), ((rows, hp), BF16), ((rows, hp), BF16),
            ((hp, width), BF16), ((8, width), F32),
            ((nb, 8, width), F32), ((nb, STATE, width), BF16),
            ((nj, STATE, LANES), BF16), ((nj, 8, LANES), F32), ((nj, STATE, LANES), BF16), ((nj, 8, LANES), F32),
            ((nj, STATE, LANES), BF16), ((nj, STATE, LANES), BF16), ((nj, STATE, LANES), BF16),
            ((nj, STATE, LANES), BF16),
            ((rows, width), F32), ((rows, width), F32), ((rows, width), BF16), ((rows, LANES), F32),
            ((every, own, COLS), BF16), ((every, own, COLS), BF16), ((every, own, COLS), F32),
            ((far, own, COLS), BF16), ((far, own, COLS), BF16),
            ((n_head, 8, own), F32), ((n_head, 8, own), F32),
        ]
        sems = [4, 2, 2] + [nj] * 8 + [every, every, far, far, n_head, n_head]
        return pl.pallas_call(
            functools.partial(kernel, n_seq, n_head, norm_weight.shape[0]),
            out_shape=jax.ShapeDtypeStruct((own, d_model), BF16),
            in_specs=[hbm] * 4 + [vmem] * 7,
            out_specs=vmem,
            scratch_shapes=[pltpu.VMEM(*one) for one in scratch] + [dma((k,)) for k in sems],
            compiler_params=pltpu.CompilerParams(
                collective_id=0, has_side_effects=True, vmem_limit_bytes=60 * 2**20
            ),
        )(
            x_in, z_gate, bc_in, w_out, conv_x, conv_bc, dt_raw, dt_bias[None], a_log[None],
            skip_d[None], norm_weight.reshape(n_head, 1, width),
        )

    in_specs = (
        P("seq", "head"), P("seq", "head"), P("seq", None), P(None, "head"), P(), P("head", "seq"),
        P("head"), P("head"), P("head"), P(), P("head", None),
    )
    return jax.shard_map(
        per_device, mesh=mesh, in_specs=in_specs, out_specs=P(("seq", "head"), None), check_vma=False
    )
```

```python
import functools

import jax
import jax.numpy as jnp
from jax import lax
from jax.experimental import pallas as pl
from jax.experimental.pallas import tpu as pltpu
from jax.sharding import PartitionSpec as P

HEAD_DIM = 64
STATE = 128
CONV = 4
GROUP = 128
LANES = 128
HALO = 16
COLS = 512
LAG = 4
EPSILON = 1e-05
MESH = pl.DeviceIdType.MESH
F32 = jnp.float32
BF16 = jnp.bfloat16
HIGH = lax.Precision.HIGHEST


def silu(v):
    half = 0.5 * v
    return half + half * jnp.tanh(half)


def dot(a, b):
    return jnp.dot(a, b, preferred_element_type=F32)


def dot_nt(a, b):
    return lax.dot_general(a, b, (((1,), (1,)), ((), ())), precision=HIGH, preferred_element_type=F32)


def split(v):
    high = v.astype(BF16)
    return high, (v - high.astype(F32)).astype(BF16)


def kernel(
    n_seq, n_head, d_inner,
    x_hbm, z_hbm, bc_hbm, w_hbm, convx, convbc, dt_raw, dt_bias, a_log, skip, gain,
    out,
    xv, zv, bcv, wv, tx, tbc, hx, hbc, xf, bcf, xs, cs, bt, dts, las, cum_t, row_t, te_b, end_hi, end_lo, ef_hi, ef_lo, emat, skipx,
    pre, est, hl, dm, hpart, dpart, prev, psend, csend, inc, aa, bf, gn, acc,
    tosib, fromsib, keep, ysend, yrecv, ssend, srecv,
    load_sem, halo_send, halo_recv, a_send, a_recv, d_send, d_recv, b_send, b_recv, c_send, c_recv,
    sib_send, sib_recv, y_send, y_recv, s_send, s_recv,
):
    rows, width = xv.shape
    heads = dt_raw.shape[0]
    hp = las.shape[0]
    nb, nj = rows // GROUP, width // LANES
    d_model = wv.shape[1]
    own = out.shape[0]
    ncol = d_model // COLS
    n_chip = n_head // 2
    s = lax.axis_index("seq")
    hid = lax.axis_index("head")
    par, pair, npair = lax.rem(s, 2), s // 2, n_seq // 2
    partner = s + 1 - 2 * par
    chip, core = hid // 2, lax.rem(hid, 2)
    sibling = hid + 1 - 2 * core

    tails = [
        pltpu.make_async_copy(bc_hbm.at[pl.ds(rows - HALO, HALO)], tbc, load_sem.at[4]),
        pltpu.make_async_copy(x_hbm.at[pl.ds(rows - HALO, HALO)], tx, load_sem.at[5]),
    ]
    loads = [
        pltpu.make_async_copy(bc_hbm, bcv, load_sem.at[0]),
        pltpu.make_async_copy(x_hbm, xv, load_sem.at[1]),
        pltpu.make_async_copy(z_hbm, zv, load_sem.at[2]),
        pltpu.make_async_copy(w_hbm, wv, load_sem.at[3]),
    ]
    for load in tails + loads:
        load.start()

    barrier = pltpu.get_barrier_semaphore()
    count = 0
    for off in (-2, -1, 1, 2):
        there = jnp.logical_and(s + off >= 0, s + off < n_seq)

        @pl.when(there)
        def _():
            pl.semaphore_signal(barrier, inc=1, device_id={"seq": s + off}, device_id_type=MESH)

        count = count + jnp.where(there, 1, 0)
    for d in range(1, n_head):
        pl.semaphore_signal(
            barrier, inc=1, device_id={"head": lax.rem(hid + d, n_head)}, device_id_type=MESH
        )
    for tail in tails:
        tail.wait()
    pl.semaphore_wait(barrier, count + n_head - 1)

    def remote(src, dst, send, recv, axis, to):
        return pltpu.make_async_remote_copy(
            src_ref=src, dst_ref=dst, send_sem=send, recv_sem=recv,
            device_id={axis: to}, device_id_type=MESH,
        )

    halo_x = remote(tx, hx, halo_send.at[0], halo_recv.at[0], "seq", s + 1)
    halo_b = remote(tbc, hbc, halo_send.at[1], halo_recv.at[1], "seq", s + 1)

    @pl.when(s < n_seq - 1)
    def _():
        halo_b.start()
        halo_x.start()

    @pl.when(s == 0)
    def _():
        hx[...] = jnp.zeros_like(hx)
        hbc[...] = jnp.zeros_like(hbc)

    @pl.when(pair == 0)
    def _():
        prev[...] = jnp.zeros_like(prev)

    same = lax.broadcasted_iota(jnp.int32, (heads, heads), 0) == lax.broadcasted_iota(jnp.int32, (heads, heads), 1)

    def column(row):
        return jnp.sum(jnp.where(same, row[...], 0.0), axis=1, keepdims=True)

    raw = dt_raw[...] + column(dt_bias)
    dt = jnp.maximum(raw, 0.0) + jnp.log(1.0 + jnp.exp(-jnp.abs(raw)))
    dts[...] = jnp.ones_like(dts)
    las[...] = jnp.zeros_like(las)
    dts[0:heads, :] = dt
    las[0:heads, :] = dt * (-jnp.exp(column(a_log)))
    ti = lax.broadcasted_iota(jnp.int32, (GROUP, GROUP), 0)
    si = lax.broadcasted_iota(jnp.int32, (GROUP, GROUP), 1)
    causal = ti >= si
    tri = causal.astype(F32)
    eye = (ti == si).astype(F32)
    emat[...] = (
        lax.broadcasted_iota(jnp.int32, (hp, width), 1) // HEAD_DIM
        == lax.broadcasted_iota(jnp.int32, (hp, width), 0)
    ).astype(F32).astype(BF16)
    for c in range(nb):
        blk = slice(c * GROUP, (c + 1) * GROUP)
        dt_c, la_c = dts[:, blk], las[:, blk]
        cum = dot_nt(tri, la_c)
        cum_t[blk, :] = cum
        row_t[c] = dot_nt(la_c, tri) - jnp.log(dt_c)
        te = jnp.exp(cum[GROUP - 1 :, :] - cum) * dot_nt(eye, dt_c)
        te_b[blk, :] = te.astype(BF16)
        grown = jnp.exp(cum)
        ef_hi[blk, :], ef_lo[blk, :] = split(grown)
        end_hi[c], end_lo[c] = split(jnp.broadcast_to(grown[GROUP - 1 :, :], end_hi.shape[1:]))
    sk = jnp.where(
        lax.broadcasted_iota(jnp.int32, (heads, width), 1) // HEAD_DIM
        == lax.broadcasted_iota(jnp.int32, (heads, width), 0),
        column(skip), 0.0,
    )
    skipx[...] = jnp.broadcast_to(jnp.sum(sk, axis=0, keepdims=True), skipx.shape)

    loads[0].wait()
    loads[1].wait()

    @pl.when(s > 0)
    def _():
        halo_b.wait_recv()
        halo_x.wait_recv()

    bcf[0:8, :] = hbc[...].astype(F32)[HALO - 8 :]
    bcf[8:, :] = bcv[...].astype(F32)
    conv = convbc[0:1, :] * bcf[pl.ds(9 - CONV, rows), :]
    for k in range(1, CONV):
        conv = conv + convbc[k : k + 1, :] * bcf[pl.ds(9 - CONV + k, rows), :]
    bcs = silu(conv).astype(BF16)
    cs[...] = bcs[:, STATE:]
    for c in range(nb):
        bt[c] = bcs[c * GROUP : (c + 1) * GROUP, :STATE].astype(F32).T.astype(BF16)

    def sends_a(j):
        return (
            remote(hl.at[j], hpart.at[j], a_send.at[j], a_recv.at[j], "seq", partner),
            remote(dm.at[j], dpart.at[j], d_send.at[j], d_recv.at[j], "seq", partner),
        )

    def send_b(j):
        return remote(psend.at[j], prev.at[j], b_send.at[j], b_recv.at[j], "seq", s + 2)

    def send_c(j):
        return remote(csend.at[j], inc.at[j], c_send.at[j], c_recv.at[j], "seq", partner)

    def lanes_of(j):
        return pl.ds(pl.multiple_of(j * LANES, LANES), LANES)

    def serve(i, carry):
        j = 2 * i + par
        for copy in sends_a(j):
            copy.wait_recv()

        @pl.when(pair > 0)
        def _():
            send_b(j).wait_recv()

        first = par == 0
        h_me, h_other = hl[j].astype(F32), hpart[j].astype(F32)
        d_me, d_other = dm[j, 0:1, :], dpart[j, 0:1, :]
        h0, h1 = jnp.where(first, h_me, h_other), jnp.where(first, h_other, h_me)
        d0, d1 = jnp.where(first, d_me, d_other), jnp.where(first, d_other, d_me)
        in0 = prev[j].astype(F32)
        in1 = d0 * in0 + h0

        @pl.when(pair < npair - 1)
        def _():
            psend[j] = (d1 * in1 + h1).astype(BF16)
            send_b(j).start()

        csend[j] = jnp.where(first, in1, in0).astype(BF16)
        send_c(j).start()
        inc[j] = jnp.where(first, in0, in1).astype(BF16)
        return carry

    def own_state(j, carry):
        ln = lanes_of(j)
        xf[0:8, :] = hx[:, ln].astype(F32)[HALO - 8 :]
        xf[8:, :] = xv[:, ln].astype(F32)
        cx = convx[:, ln]
        total = cx[0:1, :] * xf[pl.ds(9 - CONV, rows), :]
        for k in range(1, CONV):
            total = total + cx[k : k + 1, :] * xf[pl.ds(9 - CONV + k, rows), :]
        xb = silu(total).astype(BF16)
        xs[:, ln] = xb
        em = emat[:, ln]
        u = (xb.astype(F32) * dot(te_b[...], em)).astype(BF16)
        run = jnp.zeros((STATE, LANES), F32)
        carried = jnp.ones((1, LANES), F32)
        for c in range(nb):
            blk = slice(c * GROUP, (c + 1) * GROUP)
            est[c, :, ln] = run.astype(BF16)
            pre[c, :, ln] = jnp.broadcast_to(carried, (8, LANES))
            decay = (dot(end_hi[c], em) + dot(end_lo[c], em))[0:1, :]
            run = decay * run + dot(bt[c], u[blk])
            carried = carried * decay
        hl[j] = run.astype(BF16)
        dm[j] = jnp.broadcast_to(carried, (8, LANES))

        @pl.when(lax.rem(j, 2) != par)
        def _():
            for copy in sends_a(j):
                copy.start()

        late = j - LAG

        @pl.when(jnp.logical_and(pair == 0, jnp.logical_and(late >= 0, lax.rem(late + par + 2, 2) == 0)))
        def _():
            serve(late // 2, 0)

        return carry

    lax.fori_loop(0, nj, own_state, 0)
    done = jnp.where(pair == 0, (nj - LAG + 1 - par) // 2, 0)
    loads[2].wait()

    lane = lax.broadcasted_iota(jnp.int32, (GROUP, LANES), 1)

    def block(c, carry):
        tk = pl.ds(pl.multiple_of(c * GROUP, GROUP), GROUP)
        c_c = cs[tk, :]
        cb = dot(c_c, bt[c])
        cum = cum_t[tk, :]
        row = row_t[c]
        for j in range(nj):
            ln = slice(j * LANES, (j + 1) * LANES)
            x = xs[tk, ln]
            y = skipx[0:1, ln] * x.astype(F32)
            for k in range(2):
                h = 2 * j + k
                seg = cum[:, h : h + 1] - row[h : h + 1, :]
                g = (cb * jnp.exp(jnp.where(causal, seg, -1e30))).astype(BF16)
                y = y + dot(g, jnp.where((lane < HEAD_DIM) == (k == 0), x, jnp.zeros_like(x)))
            em = emat[:, ln]
            ef = dot(ef_hi[tk, :], em) + dot(ef_lo[tk, :], em)
            y = y + ef * dot(c_c, est[c, :, ln])
            sz = silu(zv[tk, ln].astype(F32))
            aa[tk, ln] = y * sz
            bf[tk, ln] = ef * pre[c, 0:1, ln] * sz
        return carry

    early = jnp.minimum(jnp.where(pair == npair - 1, pair, jnp.maximum(pair - 1, 0)), nb - 1)
    lax.fori_loop(0, early, block, 0)

    lax.fori_loop(done, nj // 2, serve, 0)
    lax.fori_loop(early, nb, block, 0)

    acc[...] = jnp.zeros_like(acc)

    chip_rows = 2 * own

    def gate(j, r):
        ln = lanes_of(j)
        tk = pl.ds(pl.multiple_of(lax.rem(chip + r, n_chip) * chip_rows, chip_rows), chip_rows)
        g = (aa[tk, ln] + bf[tk, ln] * dot(cs[tk, :], inc[j])).astype(BF16).astype(F32)
        acc[tk, :] += g * g
        gn[tk, ln] = (g * gain[hid, :, ln]).astype(BF16)

    def gate_own(i, carry):
        for r in range(n_chip):
            gate(2 * i + par, r)
        return carry

    def gate_sent(i, carry):
        j = 2 * i + 1 - par
        send_c(j).wait_recv()
        for r in range(1, n_chip):
            gate(j, r)
        return carry

    def gate_near(i, carry):
        gate(2 * i + 1 - par, 0)
        return carry

    lax.fori_loop(0, nj // 2, gate_own, 0)
    lax.fori_loop(0, nj // 2, gate_sent, 0)
    loads[3].wait()

    far = (n_chip - 1) * ncol

    def sib(e):
        return remote(tosib.at[e], fromsib.at[e], sib_send.at[e], sib_recv.at[e], "head", sibling)

    def chip_of(e):
        return lax.rem(chip + e // ncol + 1, n_chip)

    def over(e):
        return remote(ysend.at[e], yrecv.at[e], y_send.at[e], y_recv.at[e], "head", chip_of(e) * 2 + core)

    def project(e):
        base = chip_of(e) * 2
        n = lax.rem(e, ncol)
        theirs = gn[pl.ds(pl.multiple_of((base + 1 - core) * own, own), own), :]
        mine = gn[pl.ds(pl.multiple_of((base + core) * own, own), own), :]
        part = dot(
            jnp.concatenate([theirs, mine], axis=0),
            wv[:, pl.ds(pl.multiple_of(n * COLS, COLS), COLS)],
        )
        tosib[e] = part[:own].astype(BF16)
        sib(e).start()
        keep[e] = part[own:]

    def forward(e):
        sib(e).wait_recv()
        ysend[e] = (keep[e] + fromsib[e].astype(F32)).astype(BF16)
        over(e).start()

    def ssq_send(d):
        to = lax.rem(hid + d, n_head)
        return remote(ssend.at[to], srecv.at[d], s_send.at[d], s_recv.at[d], "head", to)

    def ssq_of(r):
        to_chip = lax.rem(chip + r, n_chip)
        for k in range(2):
            b = to_chip * 2 + k
            flipped = acc[pl.ds(pl.multiple_of(b * own, own), own), :].T
            ssend[b] = jnp.broadcast_to(jnp.sum(flipped, axis=0, keepdims=True), ssend.shape[1:])
        for d in range(1, n_head):

            @pl.when(lax.rem(hid + d, n_head) // 2 == to_chip)
            def _():
                ssq_send(d).start()

    for r in range(1, n_chip):
        ssq_of(r)

    def step(e, carry):
        project(e)

        @pl.when(e > 0)
        def _():
            forward(e - 1)

        return carry

    def near(e, carry):
        project(e)
        return carry

    lax.fori_loop(0, far, step, 0)
    forward(far - 1)
    lax.fori_loop(0, nj // 2, gate_near, 0)
    ssq_of(0)
    lax.fori_loop(far, far + ncol, near, 0)

    ssq = ssend[hid]
    for d in range(1, n_head):
        ssq_send(d).wait_recv()
        ssq = ssq + srecv[d]
    inv = lax.rsqrt(ssq[0:1, :] / d_inner + EPSILON)
    inv = jnp.broadcast_to(inv, (LANES, own)).T[:, 0:1]

    def finish(n, carry):
        e = far + n
        sib(e).wait_recv()
        total = keep[e] + fromsib[e].astype(F32)
        for r in range(n_chip - 1):
            over(r * ncol + n).wait_recv()
            total = total + yrecv[r * ncol + n].astype(F32)
        out[:, pl.ds(pl.multiple_of(n * COLS, COLS), COLS)] = (total * inv).astype(BF16)
        return carry

    lax.fori_loop(0, ncol, finish, 0)

    @pl.when(s < n_seq - 1)
    def _():
        halo_b.wait_send()
        halo_x.wait_send()

    def left(i, carry):
        for copy in sends_a(2 * i + 1 - par):
            copy.wait_send()
        send_c(2 * i + par).wait_send()

        @pl.when(pair < npair - 1)
        def _():
            send_b(2 * i + par).wait_send()

        return carry

    lax.fori_loop(0, nj // 2, left, 0)
    for e in range(far + ncol):
        sib(e).wait_send()
    for e in range(far):
        over(e).wait_send()
    for d in range(1, n_head):
        ssq_send(d).wait_send()


def solution(mesh):
    n_seq, n_head = mesh.shape["seq"], mesh.shape["head"]

    def per_device(x_in, z_gate, bc_in, conv_x, conv_bc, dt_raw, dt_bias, a_log, skip_d, norm_weight, w_out):
        rows, width = x_in.shape
        heads = dt_raw.shape[0]
        d_model = w_out.shape[1]
        hp = -(-heads // 32) * 32
        nb, nj, own, ncol = rows // GROUP, width // LANES, rows // n_head, d_model // COLS
        every, far = (n_head // 2) * ncol, (n_head // 2 - 1) * ncol
        assert nj % 2 == 0 and n_seq % 2 == 0 and n_head % 2 == 0 and own == LANES
        hbm, vmem = pl.BlockSpec(memory_space=pl.ANY), pl.BlockSpec(memory_space=pltpu.VMEM)
        dma = pltpu.SemaphoreType.DMA
        scratch = [
            ((rows, width), BF16), ((rows, width), BF16), ((rows, 2 * STATE), BF16), (w_out.shape, BF16),
            ((HALO, width), BF16), ((HALO, 2 * STATE), BF16), ((HALO, width), BF16), ((HALO, 2 * STATE), BF16),
            ((rows + 8, LANES), F32), ((rows + 8, 2 * STATE), F32),
            ((rows, width), BF16), ((rows, STATE), BF16), ((nb, STATE, GROUP), BF16),
            ((hp, rows), F32), ((hp, rows), F32), ((rows, hp), F32), ((nb, hp, GROUP), F32),
            ((rows, hp), BF16), ((nb, 16, hp), BF16), ((nb, 16, hp), BF16), ((rows, hp), BF16), ((rows, hp), BF16),
            ((hp, width), BF16), ((8, width), F32),
            ((nb, 8, width), F32), ((nb, STATE, width), BF16),
            ((nj, STATE, LANES), BF16), ((nj, 8, LANES), F32), ((nj, STATE, LANES), BF16), ((nj, 8, LANES), F32),
            ((nj, STATE, LANES), BF16), ((nj, STATE, LANES), BF16), ((nj, STATE, LANES), BF16),
            ((nj, STATE, LANES), BF16),
            ((rows, width), F32), ((rows, width), F32), ((rows, width), BF16), ((rows, LANES), F32),
            ((every, own, COLS), BF16), ((every, own, COLS), BF16), ((every, own, COLS), F32),
            ((far, own, COLS), BF16), ((far, own, COLS), BF16),
            ((n_head, 8, own), F32), ((n_head, 8, own), F32),
        ]
        sems = [6, 2, 2] + [nj] * 8 + [every, every, far, far, n_head, n_head]
        return pl.pallas_call(
            functools.partial(kernel, n_seq, n_head, norm_weight.shape[0]),
            out_shape=jax.ShapeDtypeStruct((own, d_model), BF16),
            in_specs=[hbm] * 4 + [vmem] * 7,
            out_specs=vmem,
            scratch_shapes=[pltpu.VMEM(*one) for one in scratch] + [dma((k,)) for k in sems],
            compiler_params=pltpu.CompilerParams(
                collective_id=0, has_side_effects=True, vmem_limit_bytes=60 * 2**20
            ),
        )(
            x_in, z_gate, bc_in, w_out, conv_x, conv_bc, dt_raw, dt_bias[None], a_log[None],
            skip_d[None], norm_weight.reshape(n_head, 1, width),
        )

    in_specs = (
        P("seq", "head"), P("seq", "head"), P("seq", None), P(None, "head"), P(), P("head", "seq"),
        P("head"), P("head"), P("head"), P(), P("head", None),
    )
    return jax.shard_map(
        per_device, mesh=mesh, in_specs=in_specs, out_specs=P(("seq", "head"), None), check_vma=False
    )
```
